32 devices in a mesh: chol: 16 (over z, x, core), virt: 2 (over y).
Axes of the slice: x: 2, y: 2, z: 4, core: 2. Of those that a mesh axis runs over, the one named last changes fastest.
Arguments:
- amplitudes: bfloat16 [9600, 600], P('chol'), may hold values from -6 to 6
- chol_vectors: bfloat16 [128, 600, 600], P('chol', 'virt'), may hold values from -0.072753906 to 0.072753906
Outputs:
- sigma: float32 [9600, 600], P('chol', 'virt')
The draws below stay inside these ranges and needn't reach their ends.
All inputs are finite; a program needn't handle non-finite values.
Results may differ from the reference program's by a relative error of at most 0.0042.
Values may be sent and summed in bfloat16 or wider, within the bound.
A program may use at most 192 MiB of HBM per device.

```python
import jax
import jax.numpy as jnp
from jax import lax

V = 600
ROOTS = 2
PAIRS = 8
CH_DEV = 8
NP = 128
N_CHOL = 16


def levels(rng, dims, split, least, high):
    def one(axis_at, parts):
        steps = jax.random.uniform(jax.random.fold_in(jax.random.fold_in(rng, 6), axis_at), (parts,), jnp.float32, least / len(split), high / len(split))
        return jnp.repeat(jnp.exp(steps), dims[axis_at] // parts).reshape((-1,) + (1,) * (len(dims) - axis_at - 1))

    gain = one(*split[0])
    for cut in split[1:]:
        gain = gain * one(*cut)
    return gain


def scatter_about(key, shape, deviation, reach, shards=(), dtype=jnp.bfloat16):
    values = deviation * jax.random.normal(key, shape, jnp.float32)
    if shards:
        values = values * levels(key, shape, shards, -0.22, 0.18)
    return jnp.clip(values, -reach, reach).astype(dtype)


def setup_inputs(seed: int = 0) -> dict:
    streams_of = jax.random.split(jax.random.key(seed), 3)
    return {
        "amplitudes": scatter_about(streams_of[0], (ROOTS * PAIRS * V, V), 1.0, 6.0, ((0, 16),)),
        "chol_vectors": scatter_about(streams_of[1], (NP, V, V), ((V * (CH_DEV * N_CHOL) ** 0.5) ** -0.5), 0.072753906, ((0, 16), (1, 2))),
    }


def reference(amplitudes, chol_vectors):
    combos = ROOTS * PAIRS

    def one_vector(running, vector):
        ladder_half = jnp.dot(amplitudes, vector.T, preferred_element_type=jnp.float32).astype(jnp.bfloat16)
        ladder_half = ladder_half.reshape(combos, V, V)
        update = jnp.einsum('ac,ncb->nab', vector.astype(jnp.float32), ladder_half.astype(jnp.float32), precision=lax.Precision.HIGHEST)
        return running + update, None

    zeros_init = jnp.zeros((combos, V, V), jnp.float32)
    total, unused = lax.scan(one_vector, zeros_init, chol_vectors)
    return total.reshape(combos * V, V)
```

```python
import functools

import jax
import jax.numpy as jnp
from jax import lax
from jax.experimental import pallas as pl
from jax.experimental.pallas import tpu as pltpu
from jax.sharding import PartitionSpec as P

MESH = pl.DeviceIdType.MESH
NT = (((1,), (1,)), ((), ()))
NN = (((1,), (0,)), ((), ()))
VMEM_LIMIT = 67043328
SIDE = 256


def up(size, unit):
    return -(-size // unit) * unit


def plain(amplitudes, chol_vectors):
    vec_count, row_share, orbitals = chol_vectors.shape
    turned = jnp.transpose(chol_vectors, (1, 2, 0)).reshape(row_share, orbitals * vec_count)
    local_flat = chol_vectors.reshape(vec_count * row_share, orbitals)
    ladder_half = jnp.dot(
        lax.all_gather(amplitudes, "chol", axis=0, tiled=True),
        local_flat.T,
        preferred_element_type=jnp.float32,
    ).astype(jnp.bfloat16)
    combos = ladder_half.shape[0] // orbitals
    half_blocks = ladder_half.reshape(combos, orbitals * vec_count, row_share)
    sigma_terms = jnp.einsum(
        "ak,nkb->nab",
        lax.all_gather(turned, "virt", axis=0, tiled=True),
        half_blocks,
        preferred_element_type=jnp.float32,
    )
    sigma_terms = sigma_terms.reshape(combos * orbitals, row_share)
    return lax.psum_scatter(sigma_terms, "chol", scatter_dimension=0, tiled=True)


def kernel(ring, r_in, l_in, out, rbuf, lbuf, xa, xb,
           mine_a, give_a, got_a, rin_a,
           mine_s, give_s, got_s, rin_s,
           mine_t, give_t, got_t, rin_t, own_s, own_t, res,
           loc_sem, h_send, h_recv, g_send, g_recv, y_send, y_recv, z_send, z_recv,
           da_send, da_recv, ds_send, ds_recv, dt_send, dt_recv,
           ra_send, ra_recv, rs_send, rs_recv, rt_send, rt_recv, f_send, f_recv):
    half = ring // 2
    chol, virt = lax.axis_index("chol"), lax.axis_index("virt")
    core, chip = chol % 2, chol // 2
    odd = chip % 2
    pos = (1 - odd) * (chip // 2) + odd * (ring - 1 - chip // 2)
    vecs, rows, width = l_in.shape
    tall = 2 * rows
    cut = tall // SIDE * SIDE
    rest = tall - cut
    first_cross = cut - rows
    hc, hr = cut // 2, rest // 2
    lane = up(rest, 128)
    pad = width - tall
    same = 1 - (core + virt) % 2
    sgn = 2 * same - 1

    def at(offset):
        there = (pos + offset + ring) % ring
        back = there // half
        q = (1 - back) * 2 * there + back * (2 * (ring - 1 - there) + 1)
        return (q * 2 + core, virt)

    partner, across = (chip * 2 + 1 - core, virt), (chol, 1 - virt)
    keeper, taker = (chip * 2 + virt, virt), (chip * 2 + virt, 1 - virt)
    peers = [at(1), at(-1), partner, across, (chip * 2 + 1 - core, 1 - virt)]

    barrier = pltpu.get_barrier_semaphore()
    for peer in peers:
        pl.semaphore_signal(barrier, inc=1, device_id=peer, device_id_type=MESH)

    cp_r = pltpu.make_async_copy(r_in, rbuf.at[0], loc_sem.at[0])
    cp_l = pltpu.make_async_copy(l_in, lbuf.at[:, pl.ds(0, rows)], loc_sem.at[1])

    @pl.when(same == 1)
    def _():
        cp_r.start()

    cp_l.start()

    @pl.loop(0, ring - 1)
    def _(d):
        xa[d, pl.ds(vecs * tall, pad), :] = jnp.zeros((pad, cut), xa.dtype)

    xb[pl.ds(vecs * tall, pad), :] = jnp.zeros((pad, 2 * lane), xb.dtype)
    cp_l.wait()

    @pl.when(same == 1)
    def _():
        cp_r.wait()

    pl.semaphore_wait(barrier, len(peers))

    def remote(src, dst, s, r, to):
        return pltpu.make_async_remote_copy(
            src_ref=src, dst_ref=dst, send_sem=s, recv_sem=r, device_id=to, device_id_type=MESH)

    def mslot(s):
        return (s * sgn + ring) % ring

    def gslot(s):
        return (ring - s * sgn) % ring

    up_rows = pl.ds(pl.multiple_of((1 - same) * rows, rows), rows)
    other_rows = pl.ds(pl.multiple_of(same * rows, rows), rows)

    def hop(s):
        return remote(rbuf.at[mslot(s - 1)], rbuf.at[mslot(s)], h_send.at[s], h_recv.at[s], at(sgn))

    def half_hop():
        return remote(rbuf.at[mslot(half - 1), up_rows], rbuf.at[half, up_rows],
                      h_send.at[half], h_recv.at[half], at(sgn))

    def give(s):
        return remote(rbuf.at[mslot(s)], rbuf.at[mslot(s)], g_send.at[s], g_recv.at[s], partner)

    def taken(s):
        return remote(rbuf.at[gslot(s)], rbuf.at[gslot(s)], g_send.at[s], g_recv.at[s], partner)

    def half_give(where):
        return remote(rbuf.at[half, where], rbuf.at[half, where], g_send.at[half], g_recv.at[half], partner)

    def cross_a(p):
        return remote(lbuf.at[p, pl.ds(0, first_cross)], lbuf.at[p, pl.ds(rows, first_cross)],
                      y_send.at[p], y_recv.at[p], across)

    def cross_b(p):
        return remote(lbuf.at[p, pl.ds(first_cross, rest)], lbuf.at[p, pl.ds(cut, rest)],
                      z_send.at[p], z_recv.at[p], across)

    for p in range(vecs):
        cross_a(p).start()
    for p in range(vecs):
        cross_b(p).start()

    own = remote(rbuf.at[0], rbuf.at[0], g_send.at[0], g_recv.at[0], partner)

    @pl.when(same == 1)
    def _():
        own.start()

    @pl.when(same == 0)
    def _():
        own.wait_recv()

    hop(1).start()

    def held(d):
        return d - 1 + half * jnp.where(d == 0, 1, 0)

    def stage_one(d, p, count, lo, hi, to=None):
        size = hi - lo
        weights = lbuf[pl.ds(p, count), lo:hi, :].reshape(count * size, width)
        y = lax.dot_general(rbuf[d], weights, NT, preferred_element_type=jnp.float32).astype(jnp.bfloat16)
        for i in range(count):
            if to is None:
                xa[held(d), pl.ds((p + i) * tall, tall), lo:hi] = y[:, i * size:(i + 1) * size]
            else:
                to[pl.ds((p + i) * tall, tall), lo:hi] = y[:, i * size:(i + 1) * size]

    def arrived(p, count):
        for q in range(p, p + count):
            cross_a(q).wait_recv()

    pair = max(vecs // 4, 1)
    stage_one(0, 0, vecs, 0, SIDE, xb)

    @pl.loop(1, half + 2)
    def _(s):
        @pl.when(s < half)
        def _():
            hop(s).wait_recv()

            @pl.when(s + 1 < half)
            def _():
                hop(s + 1).start()

            @pl.when(s + 1 == half)
            def _():
                half_hop().start()

            give(s).start()

        @pl.when(s == half)
        def _():
            half_hop().wait_recv()
            half_give(up_rows).start()
            half_give(other_rows).wait_recv()

        per = jnp.where(s < half, 2, 1)

        @pl.loop(0, jnp.where(s > half, 0, per))
        def _(t):
            @pl.when(t == 1)
            def _():
                taken(s).wait_recv()

            stage_one(((1 - 2 * t) * s * sgn + 2 * ring) % ring, 0, vecs, 0, SIDE)

        batch = jnp.where(s > half, 2, s - 1)

        @pl.when((s < 3) | (s > half))
        def _():
            for q in range(pair):
                cross_a(batch * pair + q).wait_recv()

        groups = jnp.where(s == 1, 1, jnp.where(s == 2, 3, 2))

        @pl.loop(0, jnp.where(s > half, ring - 1, groups * per))
        def _(k):
            second = jnp.where(k < per, 0, 1)
            mirror = s + second * (1 - groups + k // per)
            d = jnp.where(s > half, k + 1, mirror + k % per * (ring - 2 * mirror))
            stage_one(d, jnp.where(s > half, 2, second) * pair, pair, SIDE, cut)

    arrived(3 * pair, vecs - 3 * pair)

    def flat(base, size):
        halves = []
        for c in (core, 1 - core):
            first = pl.ds(pl.multiple_of(base + c * size, 16), size)
            halves.append(jnp.concatenate([lbuf[p, first, :] for p in range(vecs)], axis=1))
        return jnp.concatenate(halves, axis=0)

    def deep(load):
        return jnp.concatenate([load(pl.ds(p * tall, width)) for p in range(vecs)], axis=0)

    def dot(left, right):
        return lax.dot_general(left, right, NN, preferred_element_type=jnp.float32)

    def slot_of(j, t):
        return (half + j) * (1 - t) + t * ((half - j) % half)

    def pass_on(d, j, t, src, rin, s, r):
        u = (1 - t) * jnp.where(j == 0, 1 - core, 1)
        raised = (d + 1) * (1 - (d + 1) // ring) + half * ((d + 1) // ring)
        to = u * raised + (1 - u) * (d - 1)
        return remote(src, rin.at[to], s.at[d], r.at[to], at(2 * u - 1))

    def has_input(j, t):
        given = jnp.where(t == 0, 1 - core, core)
        return jnp.where(j == 0, 0, jnp.where(j == 1, given, 1)) == 1

    def incoming(rin, s, r, d):
        return remote(rin.at[d], rin.at[d], s.at[d], r.at[d], at(1))

    def turn(i):
        if isinstance(i, int):
            return ((i + 1) // 2, (i + 1) % 2 if i else 0)
        return (i + 1) // 2, (i + 1) % 2 * jnp.where(i == 0, 0, 1)

    def a_slot(i):
        j, t = turn(i)
        return slot_of(j, t) % ring

    def hand_a(i):
        d = a_slot(i)
        return remote(give_a.at[i % 2], got_a.at[d], da_send.at[i % 2], da_recv.at[d], partner)

    def combine_a(i):
        j, t = turn(i)
        d = a_slot(i)
        hand_a(i).wait_recv()

        @pl.when(has_input(j, t))
        def _():
            incoming(rin_a, ra_send, ra_recv, d).wait_recv()
            mine_a[i % 2] += rin_a[d].astype(jnp.float32)

        got_a[d] = (mine_a[i % 2] + got_a[d].astype(jnp.float32)).astype(jnp.bfloat16)
        pass_on(d, j, t, got_a.at[d], rin_a, ra_send, ra_recv).start()

    def big(i, d):
        total = None
        for p in range(0, vecs, 2):
            left = jnp.concatenate([jnp.concatenate([lbuf[q, pl.ds(pl.multiple_of(c * hc, 16), hc), :]
                                                     for q in (p, p + 1)], axis=1) for c in (core, 1 - core)], axis=0)
            right = jnp.concatenate([xa[held(d), pl.ds(q * tall, width), :] for q in (p, p + 1)], axis=0)
            o = dot(left, right)
            total = o if total is None else total + o
        mine_a[i % 2] = total[:hc]
        give_a[i % 2] = total[hc:].astype(jnp.bfloat16)
        hand_a(i).start()

    def strip(j, t):
        o = dot(flat(cut, hr), deep(lambda k: xa[held(slot_of(j, t)), k, :]))
        mine_t[j % 2, t] = o[:hr]
        give_t[j % 2, t] = o[hr:].astype(jnp.bfloat16)

    @pl.loop(0, ring - 1)
    def _(i):
        d = a_slot(i)
        stage_one(d, 3 * pair, vecs - 3 * pair, SIDE, cut)

        @pl.when(i >= 2)
        def _():
            hand_a(i - 2).wait_send()

        big(i, d)

        @pl.when(i > 0)
        def _():
            combine_a(i - 1)

    for p in range(vecs):
        cross_b(p).wait_recv()

    final = ring - 1

    @pl.loop(0, 1)
    def _(t):
        strip(0, t)

    combine_a(final - 1)

    @pl.loop(0, vecs)
    def _(p):
        where = pl.ds(pl.multiple_of(p * tall, 16), tall)
        xa[half - 1, where, 0:SIDE] = xb[where, :]

    @pl.loop(0, 2)
    def _(k):
        stage_one(0, k * (vecs // 2), vecs // 2, SIDE, cut)

    hand_a(final - 2).wait_send()

    @pl.loop(final, final + 1)
    def _(i):
        big(i, a_slot(i))

    mine_rows_a = pl.ds(pl.multiple_of(core * hc, 16), hc)
    mine_rows_t = pl.ds(pl.multiple_of(cut + core * hr, 16), hr)
    mine_rows_s = pl.ds(pl.multiple_of(core * rows, 16), rows)
    keep_w = up(rows, 128)
    low = rows // 128 * 128

    far_a = remote(mine_a.at[final % 2, :, pl.ds(low, cut - low)], res.at[mine_rows_a, pl.ds(0, cut - low)],
                   f_send.at[0], f_recv.at[3 * core], taker)
    by_a = remote(mine_a.at[final % 2, :, pl.ds(0, keep_w)], res.at[mine_rows_a, pl.ds(0, keep_w)],
                  f_send.at[3], f_recv.at[0], keeper)

    def finish_a():
        hand_a(final).wait_recv()
        for d in (0, half):
            incoming(rin_a, ra_send, ra_recv, d).wait_recv()
        mine_a[final % 2] += (got_a[0].astype(jnp.float32) + rin_a[0].astype(jnp.float32)
                              + rin_a[half].astype(jnp.float32))
        far_a.start()

        @pl.when(same == 0)
        def _():
            by_a.start()

        @pl.when(same == 1)
        def _():
            res[mine_rows_a, 0:keep_w] = mine_a[final % 2, :, 0:keep_w]

    def hand_s(j):
        return remote(give_s.at[j % 2], got_s.at[j], ds_send.at[j % 2], ds_recv.at[j], partner)

    def hand_t(j):
        return remote(give_t.at[j % 2], got_t.at[j], dt_send.at[j % 2], dt_recv.at[j], partner)

    def combine_b(j, t):
        d = slot_of(j, t)
        cols = slice(t * lane, (t + 1) * lane)

        if t == 1:
            @pl.when(j == 0)
            def _():
                own_s[...] = mine_s[0, :, cols] + got_s[0, :, cols].astype(jnp.float32)
                own_t[...] = mine_t[0, t] + got_t[0, t].astype(jnp.float32)

        @pl.when(has_input(j, t))
        def _():
            incoming(rin_s, rs_send, rs_recv, d).wait_recv()
            incoming(rin_t, rt_send, rt_recv, d).wait_recv()
            mine_s[j % 2, :, cols] += rin_s[d].astype(jnp.float32)
            mine_t[j % 2, t] += rin_t[d].astype(jnp.float32)

        @pl.when(d != 0)
        def _():
            got_s[j, :, cols] = (mine_s[j % 2, :, cols] + got_s[j, :, cols].astype(jnp.float32)).astype(jnp.bfloat16)
            got_t[j, t] = (mine_t[j % 2, t] + got_t[j, t].astype(jnp.float32)).astype(jnp.bfloat16)
            pass_on(d, j, t, got_s.at[j, :, pl.ds(t * lane, lane)], rin_s, rs_send, rs_recv).start()
            pass_on(d, j, t, got_t.at[j, t], rin_t, rt_send, rt_recv).start()

    def handed(j):
        hand_s(j).wait_recv()
        hand_t(j).wait_recv()

    @pl.loop(0, half)
    def _(j):
        @pl.loop(0, 2)
        def _(t):
            d = slot_of(j, t)
            pieces = []
            for p in range(vecs):
                pieces.append(lbuf[p, cut:tall, :])
                if lane > rest:
                    pieces.append(jnp.zeros((lane - rest, width), lbuf.dtype))
            y = lax.dot_general(rbuf[d], jnp.concatenate(pieces, axis=0), NT,
                                preferred_element_type=jnp.float32).astype(jnp.bfloat16)
            for p in range(vecs):
                xb[pl.ds(p * tall, tall), pl.ds(pl.multiple_of(t * lane, lane), lane)] = y[:, p * lane:(p + 1) * lane]

        @pl.when(j >= 2)
        def _():
            hand_s(j - 2).wait_send()
            hand_t(j - 2).wait_send()

        @pl.loop(0, 2)
        def _(t):
            @pl.when(j + t > 0)
            def _():
                strip(j, t)

        hand_t(j).start()

        @pl.loop(0, 1)
        def _(t):
            o = dot(flat(0, rows), deep(lambda k: xb[k, :]))
            mine_s[j % 2] = o[:rows]
            give_s[j % 2] = o[rows:].astype(jnp.bfloat16)

        hand_s(j).start()

        @pl.when(j == 1)
        def _():
            finish_a()

        @pl.when(j > 0)
        def _():
            handed(j - 1)
            for t in range(2):
                combine_b(j - 1, t)

    end = half - 1
    handed(end)
    for t in range(2):
        combine_b(end, t)
    for d in (0, half):
        incoming(rin_s, rs_send, rs_recv, d).wait_recv()
        incoming(rin_t, rt_send, rt_recv, d).wait_recv()
    own_s[...] += rin_s[0].astype(jnp.float32) + rin_s[half].astype(jnp.float32)
    own_t[...] += rin_t[0].astype(jnp.float32) + rin_t[half].astype(jnp.float32)
    far_s = remote(own_s, res.at[mine_rows_s, pl.ds(cut - low, lane)],
                   f_send.at[2], f_recv.at[3 * core + 2], taker)
    far_t = remote(own_t.at[:, pl.ds(low, cut - low)], res.at[mine_rows_t, pl.ds(0, cut - low)],
                   f_send.at[1], f_recv.at[3 * core + 1], taker)
    by_t = remote(own_t.at[:, pl.ds(0, keep_w)], res.at[mine_rows_t, pl.ds(0, keep_w)],
                  f_send.at[4], f_recv.at[1], keeper)
    far_s.start()
    far_t.start()

    @pl.when(same == 0)
    def _():
        by_t.start()
        for c in range(2):
            rows_a = pl.ds(c * hc, hc)
            rows_t = pl.ds(cut + c * hr, hr)
            rows_s = pl.ds(c * rows, rows)
            ref = res.at[rows_a, pl.ds(0, cut - low)]
            remote(ref, ref, f_send.at[0], f_recv.at[3 * c], across).wait_recv()
            ref = res.at[rows_t, pl.ds(0, cut - low)]
            remote(ref, ref, f_send.at[1], f_recv.at[3 * c + 1], across).wait_recv()
            ref = res.at[rows_s, pl.ds(cut - low, lane)]
            remote(ref, ref, f_send.at[2], f_recv.at[3 * c + 2], across).wait_recv()
        by_a.wait_send()
        by_t.wait_send()

    @pl.when(same == 1)
    def _():
        res[mine_rows_t, 0:keep_w] = own_t[:, 0:keep_w]
        other_a = pl.ds(pl.multiple_of((1 - core) * hc, 16), hc)
        other_t = pl.ds(pl.multiple_of(cut + (1 - core) * hr, 16), hr)
        ref = res.at[other_a, pl.ds(0, keep_w)]
        remote(ref, ref, f_send.at[3], f_recv.at[0], partner).wait_recv()
        ref = res.at[other_t, pl.ds(0, keep_w)]
        remote(ref, ref, f_send.at[4], f_recv.at[1], partner).wait_recv()

    for c in range(2):
        dst = (core * (1 - c) + (1 - core) * c) * rows
        cp = pltpu.make_async_copy(res.at[pl.ds(c * rows, rows)],
                                   out.at[pl.ds(pl.multiple_of(dst, 16), rows)], loc_sem.at[c])
        cp.start()

    far_a.wait_send()
    far_s.wait_send()
    far_t.wait_send()
    for i in (ring - 2, ring - 1):
        hand_a(i).wait_send()
    for j in (half - 2, half - 1):
        hand_s(j).wait_send()
        hand_t(j).wait_send()
    for d in range(1, ring):
        remote(got_a.at[d], rin_a.at[d], ra_send.at[d], ra_recv.at[d], partner).wait_send()
        remote(rin_s.at[d], rin_s.at[d], rs_send.at[d], rs_recv.at[d], partner).wait_send()
        remote(rin_t.at[d], rin_t.at[d], rt_send.at[d], rt_recv.at[d], partner).wait_send()
    for s in range(1, half):
        hop(s).wait_send()
        give(s).wait_send()
    half_hop().wait_send()
    half_give(up_rows).wait_send()
    for p in range(vecs):
        cross_a(p).wait_send()
        cross_b(p).wait_send()

    @pl.when(same == 1)
    def _():
        own.wait_send()

    for c in range(2):
        dst = (core * (1 - c) + (1 - core) * c) * rows
        pltpu.make_async_copy(res.at[pl.ds(c * rows, rows)],
                              out.at[pl.ds(pl.multiple_of(dst, 16), rows)], loc_sem.at[c]).wait()


def scratch(ring, vecs, share, orbitals):
    rows, width = up(share, 16), up(orbitals, 128)
    tall, half = 2 * rows, ring // 2
    cut = tall // SIDE * SIDE
    rest = tall - cut
    lane = up(rest, 128)
    keep_w = max(up(rows, 128), cut - rows // 128 * 128 + lane)
    deep = vecs * tall + width - tall
    bf, f32 = jnp.bfloat16, jnp.float32
    return [
        ((ring, tall, width), bf), ((vecs, tall, width), bf),
        ((ring - 1, deep, cut), bf), ((deep, 2 * lane), bf),
        ((2, cut // 2, cut), f32), ((2, cut // 2, cut), bf), ((ring, cut // 2, cut), bf), ((ring, cut // 2, cut), bf),
        ((2, rows, 2 * lane), f32), ((2, rows, 2 * lane), bf), ((half, rows, 2 * lane), bf), ((ring, rows, lane), bf),
        ((2, 2, rest // 2, cut), f32), ((2, 2, rest // 2, cut), bf), ((half, 2, rest // 2, cut), bf),
        ((ring, rest // 2, cut), bf),
        ((rows, lane), f32), ((rest // 2, cut), f32), ((tall, keep_w), f32),
    ]


def fits(chol, virt, amplitudes, chol_vectors):
    vecs, share, orbitals = chol_vectors.shape
    if virt != 2 or chol % 4 or chol < 16 or vecs % 4:
        return False
    if amplitudes.shape[0] != orbitals or 2 * share != orbitals:
        return False
    rows = up(share, 16)
    cut = 2 * rows // SIDE * SIDE
    if cut != 2 * SIDE or 2 * up(2 * rows - cut, 128) != SIDE or rows < SIDE or cut <= rows or (2 * rows - cut) % 32 or up(orbitals, 128) <= 2 * rows:
        return False
    used = 0
    for shape, kind in scratch(chol // 2, vecs, share, orbitals):
        size = jnp.dtype(kind).itemsize
        for n in shape:
            size *= n
        used += size
    return used < VMEM_LIMIT


def fused(ring, amplitudes, chol_vectors):
    vecs, share, orbitals = chol_vectors.shape
    rows, width = up(share, 16), up(orbitals, 128)
    tall, half = 2 * rows, ring // 2
    r = jnp.pad(amplitudes, ((0, tall - orbitals), (0, width - orbitals)))
    l = jnp.pad(chol_vectors, ((0, 0), (0, rows - share), (0, width - orbitals)))
    dma = pltpu.SemaphoreType.DMA
    bufs = [pltpu.VMEM(shape, kind) for shape, kind in scratch(ring, vecs, share, orbitals)]
    shape = scratch(ring, vecs, share, orbitals)[-1][0]
    turned = pl.pallas_call(
        functools.partial(kernel, ring),
        out_shape=jax.ShapeDtypeStruct(shape, jnp.float32),
        in_specs=[pl.BlockSpec(memory_space=pl.ANY)] * 2,
        out_specs=pl.BlockSpec(memory_space=pl.ANY),
        scratch_shapes=bufs + [
            dma((2,)), dma((half + 1,)), dma((half + 1,)), dma((half + 1,)), dma((half + 1,)),
            dma((vecs,)), dma((vecs,)), dma((vecs,)), dma((vecs,)),
            dma((2,)), dma((ring,)), dma((2,)), dma((half,)), dma((2,)), dma((half,)),
            dma((ring,)), dma((ring,)), dma((ring,)), dma((ring,)), dma((ring,)), dma((ring,)),
            dma((5,)), dma((6,)),
        ],
        compiler_params=pltpu.CompilerParams(
            collective_id=0, has_side_effects=True, vmem_limit_bytes=VMEM_LIMIT),
        name="ladder",
    )(r, l)
    skip = rows % 128
    here = lax.axis_index("chol") % 2 == lax.axis_index("virt")
    sides = jnp.where(here, turned[:, :share], turned[:, skip:skip + share])
    return jnp.concatenate([sides[:share], sides[rows:rows + share]], axis=0)


def solution(mesh):
    chol, virt = mesh.shape["chol"], mesh.shape["virt"]

    def shards(amplitudes, chol_vectors):
        if fits(chol, virt, amplitudes, chol_vectors):
            return fused(chol // 2, amplitudes, chol_vectors)
        return plain(amplitudes, chol_vectors)

    placed = (P("chol", None), P("chol", "virt", None))
    return jax.shard_map(
        shards, mesh=mesh, in_specs=placed, out_specs=P("chol", "virt"), check_vma=False
    )
```

```python
import functools

import jax
import jax.numpy as jnp
from jax import lax
from jax.experimental import pallas as pl
from jax.experimental.pallas import tpu as pltpu
from jax.sharding import PartitionSpec as P

MESH = pl.DeviceIdType.MESH
NT = (((1,), (1,)), ((), ()))
NN = (((1,), (0,)), ((), ()))
VMEM_LIMIT = 67043328
SIDE = 256


def up(size, unit):
    return -(-size // unit) * unit


def plain(amplitudes, chol_vectors):
    vec_count, row_share, orbitals = chol_vectors.shape
    turned = jnp.transpose(chol_vectors, (1, 2, 0)).reshape(row_share, orbitals * vec_count)
    local_flat = chol_vectors.reshape(vec_count * row_share, orbitals)
    ladder_half = jnp.dot(
        lax.all_gather(amplitudes, "chol", axis=0, tiled=True),
        local_flat.T,
        preferred_element_type=jnp.float32,
    ).astype(jnp.bfloat16)
    combos = ladder_half.shape[0] // orbitals
    half_blocks = ladder_half.reshape(combos, orbitals * vec_count, row_share)
    sigma_terms = jnp.einsum(
        "ak,nkb->nab",
        lax.all_gather(turned, "virt", axis=0, tiled=True),
        half_blocks,
        preferred_element_type=jnp.float32,
    )
    sigma_terms = sigma_terms.reshape(combos * orbitals, row_share)
    return lax.psum_scatter(sigma_terms, "chol", scatter_dimension=0, tiled=True)


def kernel(ring, r_in, l_in, out, rbuf, lbuf, xa, xb,
           mine_a, give_a, got_a, rin_a,
           mine_s, give_s, got_s, rin_s,
           mine_t, give_t, got_t, rin_t, own_s, own_t, out_s, out_t, in_s, in_t, res,
           loc_sem, h_send, h_recv, g_send, g_recv, y_send, y_recv, z_send, z_recv,
           da_send, da_recv, ds_send, ds_recv, dt_send, dt_recv,
           ra_send, ra_recv, rs_send, rs_recv, rt_send, rt_recv, f_send, f_recv):
    half = ring // 2
    chol, virt = lax.axis_index("chol"), lax.axis_index("virt")
    core, chip = chol % 2, chol // 2
    odd = chip % 2
    pos = (1 - odd) * (chip // 2) + odd * (ring - 1 - chip // 2)
    vecs, rows, width = l_in.shape
    tall = 2 * rows
    cut = tall // SIDE * SIDE
    rest = tall - cut
    first_cross = cut - rows
    hc, hr = cut // 2, rest // 2
    lane = up(rest, 128)
    pad = width - tall
    same = 1 - (core + virt) % 2
    sgn = 2 * same - 1

    def at(offset):
        there = (pos + offset + ring) % ring
        back = there // half
        q = (1 - back) * 2 * there + back * (2 * (ring - 1 - there) + 1)
        return (q * 2 + core, virt)

    partner, across = (chip * 2 + 1 - core, virt), (chol, 1 - virt)
    keeper, taker = (chip * 2 + virt, virt), (chip * 2 + virt, 1 - virt)
    peers = [at(1), at(-1), partner, across, (chip * 2 + 1 - core, 1 - virt)]

    barrier = pltpu.get_barrier_semaphore()
    for peer in peers:
        pl.semaphore_signal(barrier, inc=1, device_id=peer, device_id_type=MESH)

    cp_r = pltpu.make_async_copy(r_in, rbuf.at[0], loc_sem.at[0])
    cp_l = pltpu.make_async_copy(l_in, lbuf.at[:, pl.ds(0, rows)], loc_sem.at[1])

    @pl.when(same == 1)
    def _():
        cp_r.start()

    cp_l.start()

    @pl.loop(0, ring - 1)
    def _(d):
        xa[d, pl.ds(vecs * tall, pad), :] = jnp.zeros((pad, cut), xa.dtype)

    xb[pl.ds(vecs * tall, pad), :] = jnp.zeros((pad, 2 * lane), xb.dtype)
    cp_l.wait()

    @pl.when(same == 1)
    def _():
        cp_r.wait()

    pl.semaphore_wait(barrier, len(peers))

    def remote(src, dst, s, r, to):
        return pltpu.make_async_remote_copy(
            src_ref=src, dst_ref=dst, send_sem=s, recv_sem=r, device_id=to, device_id_type=MESH)

    def mslot(s):
        return (s * sgn + ring) % ring

    def gslot(s):
        return (ring - s * sgn) % ring

    def rows_of(u):
        return pl.ds(pl.multiple_of(u * rows, 16), rows)

    def hop(s, u):
        return remote(rbuf.at[mslot(s - 1), rows_of(u)], rbuf.at[mslot(s), rows_of(u)],
                      h_send.at[2 * s + u], h_recv.at[2 * s + u], at(sgn))

    def give(s, u):
        ref = rbuf.at[mslot(s), rows_of(u)]
        return remote(ref, ref, g_send.at[2 * s + u], g_recv.at[2 * s + u], partner)

    def taken(s, u):
        ref = rbuf.at[gslot(s), rows_of(u)]
        return remote(ref, ref, g_send.at[2 * s + u], g_recv.at[2 * s + u], partner)

    def cross_a(p):
        return remote(lbuf.at[p, pl.ds(0, first_cross)], lbuf.at[p, pl.ds(rows, first_cross)],
                      y_send.at[p], y_recv.at[p], across)

    def cross_b(p):
        return remote(lbuf.at[p, pl.ds(first_cross, rest)], lbuf.at[p, pl.ds(cut, rest)],
                      z_send.at[p], z_recv.at[p], across)

    for p in range(vecs):
        cross_a(p).start()
    for p in range(vecs):
        cross_b(p).start()

    @pl.when(same == 1)
    def _():
        for u in range(2):
            give(0, u).start()
            hop(1, u).start()

    @pl.when(same == 0)
    def _():
        for u in range(2):
            taken(0, u).wait_recv()
            hop(1, u).start()

    def held(d):
        return d - 1 + half * jnp.where(d == 0, 1, 0)

    def stage_one(d, p, count, lo, hi, to=None):
        size = hi - lo
        weights = lbuf[pl.ds(p, count), lo:hi, :].reshape(count * size, width)
        y = lax.dot_general(rbuf[d], weights, NT, preferred_element_type=jnp.float32).astype(jnp.bfloat16)
        for i in range(count):
            if to is None:
                xa[held(d), pl.ds((p + i) * tall, tall), lo:hi] = y[:, i * size:(i + 1) * size]
            else:
                to[pl.ds((p + i) * tall, tall), lo:hi] = y[:, i * size:(i + 1) * size]

    def stage_rows(d, u):
        weights = lbuf[:, 0:SIDE, :].reshape(vecs * SIDE, width)
        y = lax.dot_general(rbuf[d, rows_of(u), :], weights, NT,
                            preferred_element_type=jnp.float32).astype(jnp.bfloat16)
        for p in range(vecs):
            where = pl.ds(pl.multiple_of(p * tall + u * rows, 16), rows)
            xa[held(d), where, 0:SIDE] = y[:, p * SIDE:(p + 1) * SIDE]

    def arrived(p, count):
        for q in range(p, p + count):
            cross_a(q).wait_recv()

    pair = max(vecs // 4, 1)
    stage_one(0, 0, vecs, 0, SIDE, xb)

    @pl.loop(1, half + 2)
    def _(s):
        per = jnp.where(s < half, 2, 1)

        @pl.loop(0, jnp.where(s > half, 0, 2 * per))
        def _(k):
            t = k % 2
            alone = t * same + (1 - t) * (1 - same)
            u = jnp.where(s < half, k // 2, alone)

            @pl.when(t == 0)
            def _():
                hop(s, u).wait_recv()

                @pl.when((s + 1 < half) | ((s + 1 == half) & (u == 1 - same)))
                def _():
                    hop(s + 1, u).start()

                give(s, u).start()

            @pl.when(t == 1)
            def _():
                taken(s, u).wait_recv()

            stage_rows(((1 - 2 * t) * s * sgn + 2 * ring) % ring, u)

        batch = jnp.where(s > half, 2, s - 1)

        @pl.when((s < 3) | (s > half))
        def _():
            for q in range(pair):
                cross_a(batch * pair + q).wait_recv()

        groups = jnp.where(s == 1, 1, jnp.where(s == 2, 3, 2))

        @pl.loop(0, jnp.where(s > half, ring - 1, groups * per))
        def _(k):
            second = jnp.where(k < per, 0, 1)
            mirror = s + second * (1 - groups + k // per)
            d = jnp.where(s > half, k + 1, mirror + k % per * (ring - 2 * mirror))
            stage_one(d, jnp.where(s > half, 2, second) * pair, pair, SIDE, cut)

    arrived(3 * pair, vecs - 3 * pair)

    def flat(base, size):
        halves = []
        for c in (core, 1 - core):
            first = pl.ds(pl.multiple_of(base + c * size, 16), size)
            halves.append(jnp.concatenate([lbuf[p, first, :] for p in range(vecs)], axis=1))
        return jnp.concatenate(halves, axis=0)

    def deep(load):
        return jnp.concatenate([load(pl.ds(p * tall, width)) for p in range(vecs)], axis=0)

    def dot(left, right):
        return lax.dot_general(left, right, NN, preferred_element_type=jnp.float32)

    def slot_of(j, t):
        return (half + j) * (1 - t) + t * ((half - j) % half)

    def pass_on(d, j, t, src, rin, s, r):
        u = (1 - t) * jnp.where(j == 0, 1 - core, 1)
        raised = (d + 1) * (1 - (d + 1) // ring) + half * ((d + 1) // ring)
        to = u * raised + (1 - u) * (d - 1)
        return remote(src, rin.at[to], s.at[d], r.at[to], at(2 * u - 1))

    def has_input(j, t):
        given = jnp.where(t == 0, 1 - core, core)
        return jnp.where(j == 0, 0, jnp.where(j == 1, given, 1)) == 1

    def incoming(rin, s, r, d):
        return remote(rin.at[d], rin.at[d], s.at[d], r.at[d], at(1))

    def turn(i):
        if isinstance(i, int):
            return ((i + 1) // 2, (i + 1) % 2 if i else 0)
        return (i + 1) // 2, (i + 1) % 2 * jnp.where(i == 0, 0, 1)

    def a_slot(i):
        j, t = turn(i)
        return slot_of(j, t) % ring

    def hand_a(i):
        d = a_slot(i)
        return remote(give_a.at[i % 2], got_a.at[d], da_send.at[i % 2], da_recv.at[d], partner)

    def combine_a(i):
        j, t = turn(i)
        d = a_slot(i)
        hand_a(i).wait_recv()

        @pl.when(has_input(j, t))
        def _():
            incoming(rin_a, ra_send, ra_recv, d).wait_recv()
            mine_a[i % 2] += rin_a[d].astype(jnp.float32)

        got_a[d] = (mine_a[i % 2] + got_a[d].astype(jnp.float32)).astype(jnp.bfloat16)
        pass_on(d, j, t, got_a.at[d], rin_a, ra_send, ra_recv).start()

    def big(i, d):
        total = None
        for p in range(0, vecs, 2):
            left = jnp.concatenate([jnp.concatenate([lbuf[q, pl.ds(pl.multiple_of(c * hc, 16), hc), :]
                                                     for q in (p, p + 1)], axis=1) for c in (core, 1 - core)], axis=0)
            right = jnp.concatenate([xa[held(d), pl.ds(q * tall, width), :] for q in (p, p + 1)], axis=0)
            o = dot(left, right)
            total = o if total is None else total + o
        mine_a[i % 2] = total[:hc]
        give_a[i % 2] = total[hc:].astype(jnp.bfloat16)
        hand_a(i).start()

    def strip(j, t):
        o = dot(flat(cut, hr), deep(lambda k: xa[held(slot_of(j, t)), k, :]))
        mine_t[j % 2, t] = o[:hr]
        give_t[j % 2, t] = o[hr:].astype(jnp.bfloat16)

    @pl.loop(0, ring - 1)
    def _(i):
        d = a_slot(i)
        stage_one(d, 3 * pair, vecs - 3 * pair, SIDE, cut)

        @pl.when(i >= 2)
        def _():
            hand_a(i - 2).wait_send()

        big(i, d)

        @pl.when(i > 0)
        def _():
            combine_a(i - 1)

    for p in range(vecs):
        cross_b(p).wait_recv()

    final = ring - 1

    @pl.loop(0, 1)
    def _(t):
        strip(0, t)

    combine_a(final - 1)

    @pl.loop(0, vecs)
    def _(p):
        where = pl.ds(pl.multiple_of(p * tall, 16), tall)
        xa[half - 1, where, 0:SIDE] = xb[where, :]

    @pl.loop(0, 2)
    def _(k):
        stage_one(0, k * (vecs // 2), vecs // 2, SIDE, cut)

    hand_a(final - 2).wait_send()

    @pl.loop(final, final + 1)
    def _(i):
        big(i, a_slot(i))

    mine_rows_a = pl.ds(pl.multiple_of(core * hc, 16), hc)
    mine_rows_t = pl.ds(pl.multiple_of(cut + core * hr, 16), hr)
    mine_rows_s = pl.ds(pl.multiple_of(core * rows, 16), rows)
    keep_w = up(rows, 128)
    low = rows // 128 * 128

    far_a = remote(mine_a.at[final % 2, :, pl.ds(low, cut - low)], res.at[mine_rows_a, pl.ds(0, cut - low)],
                   f_send.at[0], f_recv.at[3 * core], taker)
    by_a = remote(mine_a.at[final % 2, :, pl.ds(0, keep_w)], res.at[mine_rows_a, pl.ds(0, keep_w)],
                  f_send.at[3], f_recv.at[0], keeper)

    def finish_a():
        hand_a(final).wait_recv()
        for d in (0, half):
            incoming(rin_a, ra_send, ra_recv, d).wait_recv()
        mine_a[final % 2] += (got_a[0].astype(jnp.float32) + rin_a[0].astype(jnp.float32)
                              + rin_a[half].astype(jnp.float32))
        far_a.start()

        @pl.when(same == 0)
        def _():
            by_a.start()

        @pl.when(same == 1)
        def _():
            res[mine_rows_a, 0:keep_w] = mine_a[final % 2, :, 0:keep_w]

    def hand_s(j):
        return remote(give_s.at[j % 2], got_s.at[j], ds_send.at[j % 2], ds_recv.at[j], partner)

    def hand_t(j):
        return remote(give_t.at[j % 2], got_t.at[j], dt_send.at[j % 2], dt_recv.at[j], partner)

    def combine_b(j, t):
        d = slot_of(j, t)
        cols = slice(t * lane, (t + 1) * lane)

        if t == 1:
            @pl.when(j == 0)
            def _():
                own_s[...] = mine_s[0, :, cols] + got_s[0, :, cols].astype(jnp.float32)
                own_t[...] = mine_t[0, t] + got_t[0, t].astype(jnp.float32)

        @pl.when(has_input(j, t))
        def _():
            incoming(rin_s, rs_send, rs_recv, d).wait_recv()
            incoming(rin_t, rt_send, rt_recv, d).wait_recv()
            mine_s[j % 2, :, cols] += rin_s[d].astype(jnp.float32)
            mine_t[j % 2, t] += rin_t[d].astype(jnp.float32)

        @pl.when(d != 0)
        def _():
            got_s[j, :, cols] = (mine_s[j % 2, :, cols] + got_s[j, :, cols].astype(jnp.float32)).astype(jnp.bfloat16)
            got_t[j, t] = (mine_t[j % 2, t] + got_t[j, t].astype(jnp.float32)).astype(jnp.bfloat16)
            pass_on(d, j, t, got_s.at[j, :, pl.ds(t * lane, lane)], rin_s, rs_send, rs_recv).start()
            pass_on(d, j, t, got_t.at[j, t], rin_t, rt_send, rt_recv).start()

    def handed(j):
        hand_s(j).wait_recv()
        hand_t(j).wait_recv()

    @pl.loop(0, half)
    def _(j):
        @pl.loop(0, 2)
        def _(t):
            d = slot_of(j, t)
            pieces = []
            for p in range(vecs):
                pieces.append(lbuf[p, cut:tall, :])
                if lane > rest:
                    pieces.append(jnp.zeros((lane - rest, width), lbuf.dtype))
            y = lax.dot_general(rbuf[d], jnp.concatenate(pieces, axis=0), NT,
                                preferred_element_type=jnp.float32).astype(jnp.bfloat16)
            for p in range(vecs):
                xb[pl.ds(p * tall, tall), pl.ds(pl.multiple_of(t * lane, lane), lane)] = y[:, p * lane:(p + 1) * lane]

        @pl.when(j >= 2)
        def _():
            hand_s(j - 2).wait_send()
            hand_t(j - 2).wait_send()

        @pl.loop(0, 2)
        def _(t):
            @pl.when(j + t > 0)
            def _():
                strip(j, t)

        hand_t(j).start()

        @pl.loop(0, 1)
        def _(t):
            o = dot(flat(0, rows), deep(lambda k: xb[k, :]))
            mine_s[j % 2] = o[:rows]
            give_s[j % 2] = o[rows:].astype(jnp.bfloat16)

        hand_s(j).start()

        @pl.when(j == 1)
        def _():
            finish_a()

        @pl.when(j > 0)
        def _():
            handed(j - 1)
            for t in range(2):
                combine_b(j - 1, t)

    end = half - 1
    handed(end)
    for t in range(2):
        combine_b(end, t)
    for d in (0, half):
        incoming(rin_s, rs_send, rs_recv, d).wait_recv()
        incoming(rin_t, rt_send, rt_recv, d).wait_recv()
    own_s[...] += rin_s[0].astype(jnp.float32) + rin_s[half].astype(jnp.float32)
    own_t[...] += rin_t[0].astype(jnp.float32) + rin_t[half].astype(jnp.float32)
    out_s[...] = own_s[...].astype(jnp.bfloat16)
    out_t[...] = own_t[:, low:cut].astype(jnp.bfloat16)
    far_s = remote(out_s, in_s.at[mine_rows_s],
                   f_send.at[2], f_recv.at[3 * core + 2], taker)
    far_t = remote(out_t, in_t.at[pl.ds(pl.multiple_of(core * hr, 16), hr)],
                   f_send.at[1], f_recv.at[3 * core + 1], taker)
    by_t = remote(own_t.at[:, pl.ds(0, keep_w)], res.at[mine_rows_t, pl.ds(0, keep_w)],
                  f_send.at[4], f_recv.at[1], keeper)
    far_s.start()
    far_t.start()

    @pl.when(same == 0)
    def _():
        by_t.start()
        for c in range(2):
            rows_a = pl.ds(c * hc, hc)
            rows_t = pl.ds(c * hr, hr)
            rows_s = pl.ds(c * rows, rows)
            ref = res.at[rows_a, pl.ds(0, cut - low)]
            remote(ref, ref, f_send.at[0], f_recv.at[3 * c], across).wait_recv()
            ref = in_t.at[rows_t]
            remote(ref, ref, f_send.at[1], f_recv.at[3 * c + 1], across).wait_recv()
            ref = in_s.at[rows_s]
            remote(ref, ref, f_send.at[2], f_recv.at[3 * c + 2], across).wait_recv()
        res[0:tall, cut - low:cut - low + lane] = in_s[...].astype(jnp.float32)
        res[cut:tall, 0:cut - low] = in_t[...].astype(jnp.float32)
        by_a.wait_send()
        by_t.wait_send()

    @pl.when(same == 1)
    def _():
        res[mine_rows_t, 0:keep_w] = own_t[:, 0:keep_w]
        other_a = pl.ds(pl.multiple_of((1 - core) * hc, 16), hc)
        other_t = pl.ds(pl.multiple_of(cut + (1 - core) * hr, 16), hr)
        ref = res.at[other_a, pl.ds(0, keep_w)]
        remote(ref, ref, f_send.at[3], f_recv.at[0], partner).wait_recv()
        ref = res.at[other_t, pl.ds(0, keep_w)]
        remote(ref, ref, f_send.at[4], f_recv.at[1], partner).wait_recv()

    for c in range(2):
        dst = (core * (1 - c) + (1 - core) * c) * rows
        cp = pltpu.make_async_copy(res.at[pl.ds(c * rows, rows)],
                                   out.at[pl.ds(pl.multiple_of(dst, 16), rows)], loc_sem.at[c])
        cp.start()

    far_a.wait_send()
    far_s.wait_send()
    far_t.wait_send()
    for i in (ring - 2, ring - 1):
        hand_a(i).wait_send()
    for j in (half - 2, half - 1):
        hand_s(j).wait_send()
        hand_t(j).wait_send()
    for d in range(1, ring):
        remote(got_a.at[d], rin_a.at[d], ra_send.at[d], ra_recv.at[d], partner).wait_send()
        remote(rin_s.at[d], rin_s.at[d], rs_send.at[d], rs_recv.at[d], partner).wait_send()
        remote(rin_t.at[d], rin_t.at[d], rt_send.at[d], rt_recv.at[d], partner).wait_send()
    for u in range(2):
        for s in range(1, half):
            hop(s, u).wait_send()
            give(s, u).wait_send()
    hop(half, 1 - same).wait_send()
    give(half, 1 - same).wait_send()
    for p in range(vecs):
        cross_a(p).wait_send()
        cross_b(p).wait_send()

    @pl.when(same == 1)
    def _():
        for u in range(2):
            give(0, u).wait_send()

    for c in range(2):
        dst = (core * (1 - c) + (1 - core) * c) * rows
        pltpu.make_async_copy(res.at[pl.ds(c * rows, rows)],
                              out.at[pl.ds(pl.multiple_of(dst, 16), rows)], loc_sem.at[c]).wait()


def scratch(ring, vecs, share, orbitals):
    rows, width = up(share, 16), up(orbitals, 128)
    tall, half = 2 * rows, ring // 2
    cut = tall // SIDE * SIDE
    rest = tall - cut
    lane = up(rest, 128)
    keep_w = max(up(rows, 128), cut - rows // 128 * 128 + lane)
    deep = vecs * tall + width - tall
    bf, f32 = jnp.bfloat16, jnp.float32
    return [
        ((ring, tall, width), bf), ((vecs, tall, width), bf),
        ((ring - 1, deep, cut), bf), ((deep, 2 * lane), bf),
        ((2, cut // 2, cut), f32), ((2, cut // 2, cut), bf), ((ring, cut // 2, cut), bf), ((ring, cut // 2, cut), bf),
        ((2, rows, 2 * lane), f32), ((2, rows, 2 * lane), bf), ((half, rows, 2 * lane), bf), ((ring, rows, lane), bf),
        ((2, 2, rest // 2, cut), f32), ((2, 2, rest // 2, cut), bf), ((half, 2, rest // 2, cut), bf),
        ((ring, rest // 2, cut), bf),
        ((rows, lane), f32), ((rest // 2, cut), f32), ((rows, lane), bf), ((rest // 2, cut - rows // 128 * 128), bf),
        ((tall, lane), bf), ((rest, cut - rows // 128 * 128), bf), ((tall, keep_w), f32),
    ]


def fits(chol, virt, amplitudes, chol_vectors):
    vecs, share, orbitals = chol_vectors.shape
    if virt != 2 or chol % 4 or chol < 16 or vecs % 4:
        return False
    if amplitudes.shape[0] != orbitals or 2 * share != orbitals:
        return False
    rows = up(share, 16)
    cut = 2 * rows // SIDE * SIDE
    if cut != 2 * SIDE or 2 * up(2 * rows - cut, 128) != SIDE or rows < SIDE or cut <= rows or (2 * rows - cut) % 32 or up(orbitals, 128) <= 2 * rows:
        return False
    used = 0
    for shape, kind in scratch(chol // 2, vecs, share, orbitals):
        size = jnp.dtype(kind).itemsize
        for n in shape:
            size *= n
        used += size
    return used < VMEM_LIMIT


def fused(ring, amplitudes, chol_vectors):
    vecs, share, orbitals = chol_vectors.shape
    rows, width = up(share, 16), up(orbitals, 128)
    tall, half = 2 * rows, ring // 2
    r = jnp.pad(amplitudes, ((0, tall - orbitals), (0, width - orbitals)))
    l = jnp.pad(chol_vectors, ((0, 0), (0, rows - share), (0, width - orbitals)))
    dma = pltpu.SemaphoreType.DMA
    bufs = [pltpu.VMEM(shape, kind) for shape, kind in scratch(ring, vecs, share, orbitals)]
    shape = scratch(ring, vecs, share, orbitals)[-1][0]
    turned = pl.pallas_call(
        functools.partial(kernel, ring),
        out_shape=jax.ShapeDtypeStruct(shape, jnp.float32),
        in_specs=[pl.BlockSpec(memory_space=pl.ANY)] * 2,
        out_specs=pl.BlockSpec(memory_space=pl.ANY),
        scratch_shapes=bufs + [
            dma((2,)), dma((2 * half + 2,)), dma((2 * half + 2,)), dma((2 * half + 2,)), dma((2 * half + 2,)),
            dma((vecs,)), dma((vecs,)), dma((vecs,)), dma((vecs,)),
            dma((2,)), dma((ring,)), dma((2,)), dma((half,)), dma((2,)), dma((half,)),
            dma((ring,)), dma((ring,)), dma((ring,)), dma((ring,)), dma((ring,)), dma((ring,)),
            dma((5,)), dma((6,)),
        ],
        compiler_params=pltpu.CompilerParams(
            collective_id=0, has_side_effects=True, vmem_limit_bytes=VMEM_LIMIT),
        name="ladder",
    )(r, l)
    skip = rows % 128
    here = lax.axis_index("chol") % 2 == lax.axis_index("virt")
    sides = jnp.where(here, turned[:, :share], turned[:, skip:skip + share])
    return jnp.concatenate([sides[:share], sides[rows:rows + share]], axis=0)


def solution(mesh):
    chol, virt = mesh.shape["chol"], mesh.shape["virt"]

    def shards(amplitudes, chol_vectors):
        if fits(chol, virt, amplitudes, chol_vectors):
            return fused(chol // 2, amplitudes, chol_vectors)
        return plain(amplitudes, chol_vectors)

    placed = (P("chol", None), P("chol", "virt", None))
    return jax.shard_map(
        shards, mesh=mesh, in_specs=placed, out_specs=P("chol", "virt"), check_vma=False
    )
```
